32 devices in a mesh: space: 16 (over z, y, core), lat: 2 (over x).
Axes of the slice: x: 2, y: 2, z: 4, core: 2. Of those that a mesh axis runs over, the one named last changes fastest.
Arguments:
- fields: bfloat16 [4, 64, 3, 65536], P(None, None, None, ('space', 'lat')), may hold values from -6 to 6
- cell_latent: int32 [65536], P(('space', 'lat')), may hold values from 0 to 1023, as said below
- enc_weight: float32 [3, 65536], P(None, ('space', 'lat')), may hold values from -0.4375 to 0.4375
- dec_weight: float32 [3, 65536], P(None, ('space', 'lat')), may hold values from -5 to 5
- trans_weight: bfloat16 [1024, 64, 5120], P(('space', 'lat')), may hold values from -0.15625 to 0.15625
- graph_logits: float32 [1024, 5120], P(('space', 'lat')), may hold values from -6 to 6
- hidden_bias: float32 [1024, 64], P(('space', 'lat')), may hold values from -3 to 3
- out_weight: float32 [1024, 64], P(('space', 'lat')), may hold values from -0.75 to 0.75
- noise_var: float32 [1024], P(('space', 'lat')), may hold values from 0.005 to 0.05
Outputs:
- grad_enc: float32 [3, 65536], P(None, ('space', 'lat'))
- grad_dec: float32 [3, 65536], P(None, ('space', 'lat'))
- grad_trans: bfloat16 [1024, 64, 5120], P(('space', 'lat'))
- grad_graph: float32 [1024, 5120], P(('space', 'lat'))
The draws below stay inside these ranges and needn't reach their ends.
Inputs may be any that keep to these rules, and one draw needn't show every extreme that they name: `cell_latent`: cells d * 2048 to (d + 1) * 2048 - 1 are assigned latents from (d - 1) * 32 to (d + 2) * 32 - 1; for every d other than the first, the first of these cells has a latent below d * 32, and for every d other than the last, the last has one at (d + 1) * 32 or above.
All inputs are finite; a program needn't handle non-finite values.
Results may differ from the reference program's by a relative error of at most 0.0023.
The reference program's roundings to bfloat16 on the way (of `latent_bf`, `lagged`, `eff_weight` and `hidden_grad`) count: a program that leaves them out, or rounds other values in their place, can miss the bound.
Values may be sent and summed in bfloat16 or wider, within the bound.
No kernel may reach another device: no remote copies, remote signals or barrier semaphores. Data moves between devices by JAX's collectives and lax.ppermute only.
A program may use at most 192 MiB of HBM per device.

```python
import math
import jax
import jax.numpy as jnp
from jax import lax

LATENTS = 1024
HID = 64
VARS = 3
LAGS = 5
STEPS = 64
BATCH = 4
CELL_DEV = 2048
CELLS = 65536


def draw_cell_latent(key, part):
    spread_cells = CELLS // LATENTS // 2
    cell_index = jnp.arange(CELLS, dtype=jnp.int32)
    offset = jax.random.randint(key, (CELLS,), -spread_cells, spread_cells + 1, dtype=jnp.int32)
    offset = jnp.where(cell_index % CELL_DEV == 0, -spread_cells, offset)
    offset = jnp.where(cell_index % CELL_DEV == CELL_DEV - 1, spread_cells, offset)
    return jnp.clip((cell_index + offset) * LATENTS // CELLS, 0, LATENTS - 1).astype(jnp.int32)


def with_spikes(array, key, source, target, parts, factor):
    def block_of(position):
        return (jnp.arange(array.shape[position]) // (array.shape[position] // parts)).reshape((-1,) + (1,) * (array.ndim - 1 - position))

    near = jax.random.permutation(key, parts)[block_of(target)]
    far = (block_of(target) + parts // 2) % parts
    return jnp.where((block_of(source) == near) | (block_of(source) == far), factor * array, array)


def block_scale(rng, extent, pieces, smallest, top_value):
    loudness, own = 1.0, jax.random.fold_in(rng, 6)
    for axis_at, parts in pieces:
        steps = jnp.exp(jax.random.uniform(jax.random.fold_in(own, axis_at), (parts,), jnp.float32, smallest / len(pieces), top_value / len(pieces)))
        loudness = loudness * jnp.repeat(steps, extent[axis_at] // parts).reshape([-1 if axis == axis_at else 1 for axis in range(len(extent))])
    return loudness


def noise(own_key, dims, width, bound, pieces=(), kind=jnp.bfloat16):
    drawn = jax.random.normal(own_key, dims, jnp.float32) * width
    if len(pieces) > 0:
        drawn = block_scale(own_key, dims, pieces, -0.22, 0.18) * drawn
    return jnp.clip(drawn, min=-bound, max=bound).astype(kind)


def noise_with(stream_key, dims, scale, reach, cuts, heavy, held_as=jnp.bfloat16):
    drawn = scale * jax.random.normal(stream_key, dims, jnp.float32)
    if cuts:
        drawn = drawn * block_scale(stream_key, dims, cuts, -0.22, 0.18)
    return jnp.clip(with_spikes(drawn, jax.random.fold_in(stream_key, 3), *heavy), -reach, reach).astype(held_as)


def setup_inputs(seed: int = 0) -> dict:
    key_of = jax.random.split(jax.random.key(seed), 10)
    return {
        "fields": noise(key_of[0], (BATCH, STEPS, VARS, CELLS), 1.0, 6.0, ((3, 32),)),
        "cell_latent": draw_cell_latent(jax.random.fold_in(key_of[9], 71), 0),
        "enc_weight": noise(key_of[2], (VARS, CELLS), (VARS * CELLS // LATENTS) ** -0.5, 0.4375, ((1, 32),), jnp.float32),
        "dec_weight": noise(key_of[3], (VARS, CELLS), 1.0, 5.0, ((1, 32),), jnp.float32),
        "trans_weight": noise_with(key_of[4], (LATENTS, HID, LAGS * LATENTS), (LAGS * LATENTS) ** -0.5, 0.15625, ((0, 32),), (0, 2, 32, 2.75)),
        "graph_logits": noise(key_of[5], (LATENTS, LAGS * LATENTS), 1.5, 6.0, ((0, 32),), jnp.float32),
        "hidden_bias": noise(key_of[6], (LATENTS, HID), 0.5, 3.0, ((0, 32),), jnp.float32),
        "out_weight": noise(key_of[7], (LATENTS, HID), HID ** -0.5, 0.75, ((0, 32),), jnp.float32),
        "noise_var": jnp.clip(jnp.exp(math.log(0.05) - 2.3025851 * jax.random.uniform(key_of[8], (LATENTS,), jnp.float32) ** block_scale(key_of[8], (LATENTS,), ((0, 32),), -0.2, 0.2)), 0.005, 0.05),
    }


sparsity_weight = 0.01
latent_block = 64

def reference(fields, cell_latent, enc_weight, dec_weight, trans_weight, graph_logits, hidden_bias, out_weight, noise_var):
    norm_factor = 1.0 / (BATCH * STEPS)
    highest = lax.Precision.HIGHEST

    def encode(window_fields):
        projected = lax.optimization_barrier(jnp.sum(enc_weight[None] * window_fields.astype(jnp.float32), axis=1))
        return jax.ops.segment_sum(projected.T, cell_latent, num_segments=LATENTS).T
    latent = lax.map(encode, fields)
    latent_bf = latent.astype(jnp.bfloat16)

    def decode(carry, items):
        window_fields, window_latent = items
        cell_values = window_latent.astype(jnp.float32)[:, cell_latent]
        resid = dec_weight[None] * cell_values[:, None, :] - window_fields.astype(jnp.float32)
        summed = carry + lax.optimization_barrier(jnp.sum(resid * cell_values[:, None, :], axis=0))
        cell_grad = norm_factor * lax.optimization_barrier(jnp.sum(resid * dec_weight[None], axis=1))
        return (summed, jax.ops.segment_sum(cell_grad.T, cell_latent, num_segments=LATENTS).T)
    dec_total, dec_grad = lax.scan(decode, jnp.zeros((VARS, CELLS), jnp.float32), (fields, latent_bf))
    grad_dec = dec_total * norm_factor
    rows = BATCH * (STEPS - LAGS)
    lag_width = LAGS * LATENTS
    lagged = jnp.stack([latent_bf[:, LAGS - lag:STEPS - lag, :] for lag in range(1, LAGS + 1)], axis=2)
    lagged = lagged.reshape(rows, lag_width).astype(jnp.float32)
    target = latent[:, LAGS:, :].reshape(rows, LATENTS)
    blocks = LATENTS // latent_block
    items = (trans_weight.reshape(blocks, latent_block, HID, lag_width), graph_logits.reshape(blocks, latent_block, lag_width), hidden_bias.reshape(blocks, latent_block, HID), out_weight.reshape(blocks, latent_block, HID), noise_var.reshape(blocks, latent_block), target.T.reshape(blocks, latent_block, rows))

    def transit(carry, block_items):
        weights, logit_rows, biases, outs, variances, targets = block_items
        edge_prob = jax.nn.sigmoid(logit_rows)
        eff_weight = (weights.astype(jnp.float32) * edge_prob[:, None, :]).astype(jnp.bfloat16).astype(jnp.float32)
        pre_act = jnp.einsum('ri,kmi->rkm', lagged, eff_weight, precision=highest) + biases[None]
        gate_sig = jax.nn.sigmoid(pre_act)
        predicted = lax.optimization_barrier(jnp.sum(pre_act * gate_sig * outs[None], axis=2))
        direct = norm_factor * (targets.T - predicted) / variances[None]
        hidden_grad = (-direct)[:, :, None] * outs[None] * gate_sig * (1.0 + pre_act * (1.0 - gate_sig))
        hidden_grad = hidden_grad.astype(jnp.bfloat16).astype(jnp.float32)
        weight_grad = jnp.einsum('rkm,ri->kmi', hidden_grad, lagged, precision=highest)
        grad_weights = (weight_grad * edge_prob[:, None, :]).astype(jnp.bfloat16)
        flip = edge_prob * (1.0 - edge_prob)
        grad_logit = lax.optimization_barrier(jnp.sum(weight_grad * weights.astype(jnp.float32), axis=1)) * flip + sparsity_weight * flip
        carry = carry + jnp.einsum('rkm,kmi->ri', hidden_grad, eff_weight, precision=highest)
        return (carry, (grad_weights, grad_logit, direct))
    input_grad, (grad_trans, grad_graph, direct) = lax.scan(transit, jnp.zeros((rows, lag_width), jnp.float32), items)
    grad_trans = grad_trans.reshape(LATENTS, HID, lag_width)
    grad_graph = grad_graph.reshape(LATENTS, lag_width)
    direct = direct.transpose(1, 0, 2).reshape(BATCH, STEPS - LAGS, LATENTS)
    input_grad = input_grad.reshape(BATCH, STEPS - LAGS, LAGS, LATENTS)
    latent_grad = dec_grad + jnp.pad(direct, ((0, 0), (LAGS, 0), (0, 0)))
    for lag in range(1, LAGS + 1):
        latent_grad = latent_grad + jnp.pad(input_grad[:, :, lag - 1, :], ((0, 0), (LAGS - lag, lag), (0, 0)))

    def encode_grad(carry, items):
        window_fields, window_grad = items
        cell_total = window_grad[:, cell_latent]
        return (carry + lax.optimization_barrier(jnp.sum(window_fields.astype(jnp.float32) * cell_total[:, None, :], axis=0)), 0)
    grad_enc, unused = lax.scan(encode_grad, jnp.zeros((VARS, CELLS), jnp.float32), (fields, latent_grad))
    return (grad_enc, grad_dec, grad_trans, grad_graph)
```

```python
import functools

import jax
import jax.numpy as jnp
from jax import lax
from jax.experimental import pallas as pl
from jax.experimental.pallas import tpu as pltpu
from jax.sharding import PartitionSpec as P

LAGS = 5
AXES = ("space", "lat")
sparsity_weight = 0.01
f32 = jnp.float32
bf16 = jnp.bfloat16
MIB = 1 << 20


def params(mib):
    return pltpu.CompilerParams(vmem_limit_bytes=mib * MIB)


def nt_dot(a, b):
    return lax.dot_general(a, b, (((1,), (1,)), ((), ())), preferred_element_type=f32)


def pieces(x, count):
    out = []
    for _ in range(count):
        part = x.astype(bf16)
        out.append(part.astype(f32))
        x = x - out[-1]
    return out


def in_vmem(x):
    return pltpu.with_memory_space_constraint(x, pltpu.VMEM)


VMEM = pl.BlockSpec(memory_space=pltpu.VMEM)


def group_of(lat_dev):
    return 8 if lat_dev % 8 == 0 else lat_dev


def encode_kernel(loc_ref, enc_ref, dec_ref, fields_ref, enc_out, dec_out, sq_out):
    width, cells = enc_out.shape[0], loc_ref.shape[1]
    mask = lax.broadcasted_iota(jnp.int32, (width, cells), 0) == loc_ref[...]
    total, square = None, None
    for var in range(fields_ref.shape[0]):
        dec = dec_ref[var : var + 1, :]
        weights = [
            jnp.where(mask, part, 0.0).astype(bf16)
            for part in pieces(enc_ref[var : var + 1, :], 3) + pieces(dec, 2)
        ]
        part = nt_dot(jnp.concatenate(weights, axis=0), fields_ref[var])
        total = part if total is None else total + part
        square = dec * dec if square is None else square + dec * dec
    cut = [total[n * width : (n + 1) * width] for n in range(5)]
    enc_out[...] = cut[0] + (cut[1] + cut[2])
    dec_out[...] = cut[3] + cut[4]
    squares = jnp.sum(jnp.where(mask, square, 0.0), axis=1, keepdims=True)
    sq_out[...] = jnp.broadcast_to(squares, sq_out.shape)


def encode(loc, enc_weight, dec_weight, fields3, width):
    var_count, rows, cells = fields3.shape
    return pl.pallas_call(
        encode_kernel,
        in_specs=[VMEM] * 4,
        out_specs=[VMEM] * 3,
        out_shape=[jax.ShapeDtypeStruct((width, rows), f32)] * 3,
        compiler_params=params(12),
        cost_estimate=pl.CostEstimate(
            flops=50 * width * rows * cells * var_count,
            bytes_accessed=2 * rows * cells * var_count,
            transcendentals=0,
        ),
        name="encode",
    )(loc, enc_weight, dec_weight, fields3)


def edge_kernel(group, first, logit_ref, weight_ref, out_ref):
    hidden = weight_ref.shape[1]
    for k in range(group):
        edge = jax.nn.sigmoid(logit_ref[first + k : first + k + 1, :])
        out_ref[k * hidden : (k + 1) * hidden, :] = (
            weight_ref[first + k].astype(f32) * edge
        ).astype(bf16)


def effective(logits, weights, part):
    lat_dev, hidden, lag_width = weights.shape
    group = group_of(lat_dev)
    out = pl.pallas_call(
        functools.partial(edge_kernel, group, part * group),
        in_specs=[VMEM] * 2,
        out_specs=VMEM,
        out_shape=jax.ShapeDtypeStruct((group * hidden, lag_width), bf16),
        compiler_params=params(2),
        cost_estimate=pl.CostEstimate(
            flops=2 * group * hidden * lag_width,
            bytes_accessed=4 * group * hidden * lag_width,
            transcendentals=0,
        ),
        name="effective",
    )(logits, weights)
    return in_vmem(out)


def transition_kernel(steps, norm, order, inverse, parts, device_ref, lat_ref, own_ref, bias_ref,
                      out_w_ref, var_ref, dec_ref, sq_ref, *refs):
    eff = refs[:parts]
    hid_out, lagged_out, grad_out, direct_out, window_out, lagged, pre, hid_t, folded = refs[parts:]
    blocks, size, rows = lat_ref.shape
    latents = blocks * size
    span, lag_width = eff[0].shape
    lat_dev, hidden = bias_ref.shape
    group = span // hidden
    device = device_ref[0]

    def spot(block):
        found = jnp.int32(0)
        for bit, moved in inverse:
            found = found | (((block >> bit) & 1) << moved)
        return found

    for p in range(blocks):
        values = lat_ref[p].astype(f32)
        at = pl.multiple_of((device ^ order[p]) * size, size) if blocks > 1 else 0
        for lag in range(1, LAGS + 1):
            turned = pltpu.roll(values, lag, 1).astype(bf16)
            lagged[pl.ds((lag - 1) * latents + at, size), :] = turned

    bias_t, out_w_t, var_t = bias_ref[...].T, out_w_ref[...].T, var_ref[...].T
    column = lax.broadcasted_iota(jnp.int32, (group, rows), 1)
    valid = lax.rem(column, steps) >= LAGS
    for part in range(parts):
        pre[...] = jnp.dot(eff[part][...], lagged[...], preferred_element_type=f32)
        first = part * group
        for k in range(group):
            value = pre[k * hidden : (k + 1) * hidden, :] + bias_t[:, first + k : first + k + 1]
            out_w = out_w_t[:, first + k : first + k + 1]
            gate = jax.nn.sigmoid(value)
            direct_out[first + k : first + k + 1, :] = jnp.sum(
                value * gate * out_w, axis=0, keepdims=True
            )
            pre[k * hidden : (k + 1) * hidden, :] = out_w * gate * (1.0 + value * (1.0 - gate))
        at = slice(first, first + group)
        direct = norm * (own_ref[at, :] - direct_out[at, :]) / var_t[at, :]
        direct = jnp.where(valid, direct, 0.0)
        direct_out[at, :] = direct
        for k in range(group):
            here = slice(k * hidden, (k + 1) * hidden)
            slope = pre[here, :] * (-direct[k : k + 1, :])
            hid_out[part * span + k * hidden : part * span + (k + 1) * hidden, :] = slope.astype(bf16)
            pre[here, :] = slope
        hid_t[:, part * span : (part + 1) * span] = pre[...].T.astype(bf16)

    for lag in range(1, LAGS + 1):
        at = slice((lag - 1) * latents, lag * latents)
        lagged_out[:, at] = lagged[at, :].astype(f32).T.astype(bf16)
        term = None
        for part in range(parts):
            more = jnp.dot(
                hid_t[:, part * span : (part + 1) * span],
                eff[part][:, at],
                preferred_element_type=f32,
            )
            term = more if term is None else term + more
        term = pltpu.roll(term, rows - lag, 0)
        folded[...] = term if lag == 1 else folded[...] + term
    total = folded[...].T
    if blocks == 1:
        grad_out[0] = total
        return
    here = spot(device)
    for block in range(blocks):
        at = sum(((block >> bit) & 1) << moved for bit, moved in inverse)
        grad_out[at ^ here] = total[block * size : (block + 1) * size]
    grad_out[0] += direct_out[...]
    below = spot(jnp.maximum(device - 1, 0)) ^ here
    above = spot(jnp.minimum(device + 1, blocks - 1)) ^ here
    for n, at in ((0, below), (1, 0), (2, above)):
        part = slice(n * size, (n + 1) * size)
        values = lat_ref[at]
        window_out[part, :] = values
        grad_out[at] += norm * (values.astype(f32) * sq_ref[part, :] - dec_ref[part, :])


def transition(steps, norm, order, inverse, device, lat3, own, bias, out_w, var, dec_sums, squares, eff):
    blocks, size, rows = lat3.shape
    lat_dev, hidden = bias.shape
    span, lag_width = eff[0].shape
    km = lat_dev * hidden
    shape = jax.ShapeDtypeStruct
    return pl.pallas_call(
        functools.partial(transition_kernel, steps, norm, order, inverse, len(eff)),
        in_specs=[pl.BlockSpec(memory_space=pltpu.SMEM)] + [VMEM] * (7 + len(eff)),
        out_specs=[VMEM] * 5,
        out_shape=[
            shape((km, rows), bf16),
            shape((rows, lag_width), bf16),
            shape((blocks, size, rows), f32),
            shape((lat_dev, rows), f32),
            shape(dec_sums.shape, bf16),
        ],
        scratch_shapes=[
            pltpu.VMEM((lag_width, rows), bf16),
            pltpu.VMEM((span, rows), f32),
            pltpu.VMEM((rows, km), bf16),
            pltpu.VMEM((rows, blocks * size), f32),
        ],
        compiler_params=params(9),
        cost_estimate=pl.CostEstimate(
            flops=4 * km * lag_width * rows,
            bytes_accessed=2 * km * lag_width,
            transcendentals=km * rows,
        ),
        name="transition",
    )(device, lat3, own, bias, out_w, var, dec_sums, squares, *eff)


def weight_kernel(start, hid_ref, lagged_ref, logit_ref, weight_ref, *refs):
    trans_out, graph_out, work = refs[-3:]
    lat_dev, hidden, lag_width = weight_ref.shape
    tile = lagged_ref.shape[1]
    group = group_of(lat_dev)
    at = pl.multiple_of(start + pl.program_id(0) * tile, tile)
    for g in range(lat_dev // group):
        held = work.at[g % 2]
        held[...] = jnp.dot(
            hid_ref[g * group * hidden : (g + 1) * group * hidden, :],
            lagged_ref[...],
            preferred_element_type=f32,
        )
        for k in range(group):
            n = g * group + k
            edge = jax.nn.sigmoid(logit_ref[n : n + 1, :])
            grad = held[k * hidden : (k + 1) * hidden, :]
            trans_out[n] = (grad * edge).astype(bf16)
            flip = edge * (1.0 - edge)
            value = weight_ref[n, :, pl.ds(at, tile)].astype(f32)
            total = jnp.sum(grad * value, axis=0, keepdims=True)
            graph_out[n : n + 1, :] = total * flip + sparsity_weight * flip


def weight_grads(hid, lagged, logits, weights, first, count, held):
    lat_dev, hidden, lag_width = weights.shape
    km, rows = hid.shape
    tile = TILE
    group = group_of(lat_dev)
    skip = first // tile
    two = pl.BlockSpec((lat_dev, tile), lambda i: (0, i + skip))
    held = list(held)
    return pl.pallas_call(
        functools.partial(weight_kernel, first),
        grid=(count // tile,),
        in_specs=[
            pl.BlockSpec((km, rows), lambda i: (0, 0)),
            pl.BlockSpec((rows, tile), lambda i: (0, i + skip)),
            two,
            VMEM,
        ]
        + [pl.BlockSpec(memory_space=pl.ANY)] * len(held),
        out_specs=[pl.BlockSpec((lat_dev, hidden, tile), lambda i: (0, 0, i + skip)), two],
        out_shape=[
            jax.ShapeDtypeStruct(weights.shape, bf16),
            jax.ShapeDtypeStruct((lat_dev, lag_width), f32),
        ],
        scratch_shapes=[pltpu.VMEM((2, group * hidden, tile), f32)],
        input_output_aliases={4 + n: n for n in range(len(held))},
        compiler_params=params(16),
        cost_estimate=pl.CostEstimate(
            flops=2 * km * count * rows, bytes_accessed=4 * km * count, transcendentals=0
        ),
        name="weight_grads",
    )(hid, lagged, logits, weights, *held)


TILE = 256


def pick(mask, table, fields):
    both = jnp.dot(table, fields, preferred_element_type=f32)
    return jnp.sum(jnp.where(mask, both, 0.0), axis=0, keepdims=True)


def mask_of(loc_ref, width):
    return lax.broadcasted_iota(jnp.int32, (width, loc_ref.shape[1]), 0) == loc_ref[...]


def grad_dec_kernel(norm, loc_ref, win_ref, dec_ref, fields_ref, out_ref):
    values = win_ref[...]
    mask = mask_of(loc_ref, values.shape[0])
    wide = values.astype(f32)
    power = jnp.sum(wide * wide, axis=1, keepdims=True)
    power = jnp.sum(jnp.where(mask, power, 0.0), axis=0, keepdims=True)
    for var in range(fields_ref.shape[0]):
        cross = pick(mask, values, fields_ref[var])
        out_ref[var : var + 1, :] = norm * (dec_ref[var : var + 1, :] * power - cross)


def grad_enc_kernel(loc_ref, grad_ref, fields_ref, out_ref):
    high, low = (part.astype(bf16) for part in pieces(grad_ref[...], 2))
    mask = mask_of(loc_ref, high.shape[0])
    for var in range(fields_ref.shape[0]):
        out_ref[var : var + 1, :] = pick(mask, high, fields_ref[var]) + pick(
            mask, low, fields_ref[var]
        )


def cell_call(kernel, loc, table, extras, fields3, name):
    var_count, rows, cells = fields3.shape
    return pl.pallas_call(
        kernel,
        in_specs=[VMEM] * (3 + len(extras)),
        out_specs=VMEM,
        out_shape=jax.ShapeDtypeStruct((var_count, cells), f32),
        compiler_params=params(12),
        cost_estimate=pl.CostEstimate(
            flops=4 * table.shape[0] * rows * cells * var_count,
            bytes_accessed=2 * rows * cells * var_count,
            transcendentals=0,
        ),
        name=name,
    )(loc, table, *extras, fields3)


def paired(block, device, count, first):
    route = []
    for low in range(first, count - 1, 2):
        route += [(low, low + 1), (low + 1, low)]
    return lax.ppermute(block, AXES, route)


def from_neighbours(down, up, device, count):
    even = lax.rem(device, 2) == 0
    first = paired(jnp.where(even, up, down), device, count, 0)
    second = paired(jnp.where(even, down, up), device, count, 1)
    return first, second, even


def body(
    fields,
    cell_latent,
    enc_weight,
    dec_weight,
    trans_weight,
    graph_logits,
    hidden_bias,
    out_weight,
    noise_var,
):
    batch_size, step_count, var_count, cell_count = fields.shape
    lat_dev, hidden, lag_width = trans_weight.shape
    latent_count = lag_width // LAGS
    rows = batch_size * step_count
    norm = 1.0 / rows
    width = 3 * lat_dev
    space, lat = lax.axis_size("space"), lax.axis_size("lat")
    count = space * lat
    device = lax.axis_index(AXES)
    doubling = count & (count - 1) == 0 and lat_dev % 16 == 0
    bits = [n for n in range(count.bit_length() - 2, -1, -1)]
    core = lat.bit_length() - 1
    bits = [n for n in bits if n != core] + [core]

    loc = (cell_latent - (device - 1) * lat_dev)[None]
    fields3 = jnp.transpose(fields.reshape(rows, var_count, cell_count), (1, 0, 2))
    enc_sums, dec_sums, squares = encode(loc, enc_weight, dec_weight, fields3, width)
    first, second, even = from_neighbours(
        enc_sums[:lat_dev], enc_sums[2 * lat_dev :], device, count
    )
    held_weights = in_vmem(trans_weight)
    parts = lat_dev // group_of(lat_dev)
    eff = []

    def beside(value, after):
        if len(eff) == parts:
            return value
        logits, _ = lax.optimization_barrier((graph_logits, after))
        value, made = lax.optimization_barrier(
            (value, effective(logits, held_weights, len(eff)))
        )
        eff.append(made)
        return value


    own = enc_sums[lat_dev : 2 * lat_dev] + first + second
    own_bf = own.astype(bf16)

    if doubling:
        gathered = own_bf[None]
        for bit in bits:
            route = [(n, n ^ (1 << bit)) for n in range(count)]
            got = beside(lax.ppermute(gathered, AXES, route), gathered)
            gathered = jnp.concatenate([gathered, got], axis=0)
        order = [0]
        for bit in bits:
            order = order + [n ^ (1 << bit) for n in order]
        inverse = [(bit, n) for n, bit in enumerate(bits)]
    else:
        order, inverse = [0], []
        gathered = lax.all_gather(own_bf, AXES, axis=0, tiled=True)
        padded = jnp.pad(gathered, ((lat_dev, lat_dev), (0, 0)))
        window = lax.dynamic_slice_in_dim(padded, device * lat_dev, width, 0)
        gathered = gathered[None]

    while len(eff) < parts:
        gathered = beside(gathered, enc_sums)
    eff = [in_vmem(part) for part in eff]
    hid, lagged, partial, direct, seen = transition(
        step_count, norm, order, inverse, device.astype(jnp.int32)[None], gathered, own,
        hidden_bias, out_weight, noise_var[None], dec_sums, squares, eff,
    )
    window = seen if doubling else window

    if doubling:
        held = []
        total = partial
        fillers = LAGS if lag_width // LAGS % 256 == 0 else 1
        chunk = lag_width // fillers
        done = 0
        for n, bit in enumerate(reversed(bits)):
            half = total.shape[0] // 2
            route = [(m, m ^ (1 << bit)) for m in range(count)]
            got = lax.ppermute(total[half:].astype(bf16), AXES, route)
            if done < fillers:
                held = weight_grads(
                    hid, lagged, graph_logits, held_weights, done * chunk, chunk, held
                )
                done += 1
            total = total[:half] + got.astype(f32)
        while done < fillers:
            held = weight_grads(hid, lagged, graph_logits, held_weights, done * chunk, chunk, held)
            done += 1
        own_grad = total[0]
        grad_trans, grad_graph = held
    else:
        grad_trans, grad_graph = weight_grads(
            hid, lagged, graph_logits, held_weights, 0, lag_width, []
        )
        extra = norm * (window.astype(f32) * squares - dec_sums)
        extra = extra + jnp.pad(direct, ((lat_dev, lat_dev), (0, 0)))
        table = jnp.zeros((latent_count + 2 * lat_dev, rows), f32)
        table = lax.dynamic_update_slice_in_dim(table, extra, device * lat_dev, 0)
        partial = partial[0] + table[lat_dev : lat_dev + latent_count]
        own_grad = lax.psum_scatter(partial, AXES, scatter_dimension=0, tiled=True)

    grad_dec = cell_call(
        functools.partial(grad_dec_kernel, norm), loc, window, [dec_weight], fields3, "grad_dec"
    )
    first, second, even = from_neighbours(own_grad, own_grad, device, count)
    grad_window = jnp.concatenate(
        [jnp.where(even, second, first), own_grad, jnp.where(even, first, second)], axis=0
    )
    grad_enc = cell_call(grad_enc_kernel, loc, grad_window, [], fields3, "grad_enc")
    return (grad_enc, grad_dec, grad_trans, grad_graph)


def solution(mesh):
    return jax.shard_map(
        body,
        mesh=mesh,
        in_specs=(
            P(None, None, None, AXES),
            P(AXES),
            P(None, AXES),
            P(None, AXES),
            P(AXES, None, None),
            P(AXES, None),
            P(AXES, None),
            P(AXES, None),
            P(AXES),
        ),
        out_specs=(
            P(None, AXES),
            P(None, AXES),
            P(AXES, None, None),
            P(AXES, None),
        ),
        check_vma=False,
    )
```

```python
import functools

import jax
import jax.numpy as jnp
from jax import lax
from jax.experimental import pallas as pl
from jax.experimental.pallas import tpu as pltpu
from jax.sharding import PartitionSpec as P

LAGS = 5
AXES = ("space", "lat")
sparsity_weight = 0.01
f32 = jnp.float32
bf16 = jnp.bfloat16
MIB = 1 << 20


def params(mib):
    return pltpu.CompilerParams(vmem_limit_bytes=mib * MIB)


def nt_dot(a, b):
    return lax.dot_general(a, b, (((1,), (1,)), ((), ())), preferred_element_type=f32)


def pieces(x, count):
    out = []
    for _ in range(count):
        part = x.astype(bf16)
        out.append(part.astype(f32))
        x = x - out[-1]
    return out


def in_vmem(x):
    return pltpu.with_memory_space_constraint(x, pltpu.VMEM)


VMEM = pl.BlockSpec(memory_space=pltpu.VMEM)


def group_of(lat_dev):
    return 8 if lat_dev % 8 == 0 else lat_dev


def encode_kernel(loc_ref, enc_ref, dec_ref, fields_ref, enc_out, dec_out, sq_out):
    width, cells = enc_out.shape[0], loc_ref.shape[1]
    mask = lax.broadcasted_iota(jnp.int32, (width, cells), 0) == loc_ref[...]
    total, square = None, None
    for var in range(fields_ref.shape[0]):
        dec = dec_ref[var : var + 1, :]
        weights = [
            jnp.where(mask, part, 0.0).astype(bf16)
            for part in pieces(enc_ref[var : var + 1, :], 3) + pieces(dec, 2)
        ]
        part = nt_dot(jnp.concatenate(weights, axis=0), fields_ref[var])
        total = part if total is None else total + part
        square = dec * dec if square is None else square + dec * dec
    cut = [total[n * width : (n + 1) * width] for n in range(5)]
    enc_out[...] = cut[0] + (cut[1] + cut[2])
    dec_out[...] = cut[3] + cut[4]
    squares = jnp.sum(jnp.where(mask, square, 0.0), axis=1, keepdims=True)
    sq_out[...] = jnp.broadcast_to(squares, sq_out.shape)


def encode(loc, enc_weight, dec_weight, fields3, width):
    var_count, rows, cells = fields3.shape
    return pl.pallas_call(
        encode_kernel,
        in_specs=[VMEM] * 4,
        out_specs=[VMEM] * 3,
        out_shape=[jax.ShapeDtypeStruct((width, rows), f32)] * 3,
        compiler_params=params(12),
        cost_estimate=pl.CostEstimate(
            flops=50 * width * rows * cells * var_count,
            bytes_accessed=2 * rows * cells * var_count,
            transcendentals=0,
        ),
        name="encode",
    )(loc, enc_weight, dec_weight, fields3)


def edge_kernel(group, first, logit_ref, weight_ref, out_ref):
    hidden = weight_ref.shape[1]
    for k in range(group):
        edge = jax.nn.sigmoid(logit_ref[first + k : first + k + 1, :])
        out_ref[k * hidden : (k + 1) * hidden, :] = (
            weight_ref[first + k].astype(f32) * edge
        ).astype(bf16)


def effective(logits, weights, part):
    lat_dev, hidden, lag_width = weights.shape
    group = group_of(lat_dev)
    out = pl.pallas_call(
        functools.partial(edge_kernel, group, part * group),
        in_specs=[VMEM] * 2,
        out_specs=VMEM,
        out_shape=jax.ShapeDtypeStruct((group * hidden, lag_width), bf16),
        compiler_params=params(2),
        cost_estimate=pl.CostEstimate(
            flops=2 * group * hidden * lag_width,
            bytes_accessed=4 * group * hidden * lag_width,
            transcendentals=0,
        ),
        name="effective",
    )(logits, weights)
    return in_vmem(out)


def transition_kernel(steps, norm, core, order, inverse, parts, device_ref, lat_ref, own_ref, bias_ref,
                      out_w_ref, var_ref, dec_ref, sq_ref, *refs):
    eff = refs[:parts]
    hid_out, lagged_out, grad_out, direct_out, window_out, lagged, work, hid_t, folded = refs[parts:]
    blocks, size, rows = lat_ref.shape
    latents = blocks * size
    span, lag_width = eff[0].shape
    lat_dev, hidden = bias_ref.shape
    group = span // hidden
    device = device_ref[0]
    side = (device >> core) & 1

    def spot(owner):
        away = owner ^ device
        found = jnp.int32(0)
        for bit, first, second in inverse:
            found = found | (((away >> bit) & 1) << jnp.where((owner >> core) & 1, second, first))
        return found

    for p in range(blocks):
        values = lat_ref[p].astype(f32)
        at = pl.multiple_of((device ^ jnp.where(side, order[1][p], order[0][p])) * size, size)
        for lag in range(1, LAGS + 1):
            turned = pltpu.roll(values, lag, 1).astype(bf16)
            lagged[pl.ds((lag - 1) * latents + at, size), :] = turned

    bias_t, out_w_t, var_t = bias_ref[...].T, out_w_ref[...].T, var_ref[...].T
    column = lax.broadcasted_iota(jnp.int32, (group, rows), 1)
    valid = lax.rem(column, steps) >= LAGS
    for part in range(parts):
        pre = work.at[part % 2]
        pre[...] = jnp.dot(eff[part][...], lagged[...], preferred_element_type=f32)
        first = part * group
        for k in range(group):
            value = pre[k * hidden : (k + 1) * hidden, :] + bias_t[:, first + k : first + k + 1]
            out_w = out_w_t[:, first + k : first + k + 1]
            gate = jax.nn.sigmoid(value)
            direct_out[first + k : first + k + 1, :] = jnp.sum(
                value * gate * out_w, axis=0, keepdims=True
            )
            pre[k * hidden : (k + 1) * hidden, :] = out_w * gate * (1.0 + value * (1.0 - gate))
        at = slice(first, first + group)
        direct = norm * (own_ref[at, :] - direct_out[at, :]) / var_t[at, :]
        direct = jnp.where(valid, direct, 0.0)
        direct_out[at, :] = direct
        for k in range(group):
            here = slice(k * hidden, (k + 1) * hidden)
            slope = pre[here, :] * (-direct[k : k + 1, :])
            hid_out[part * span + k * hidden : part * span + (k + 1) * hidden, :] = slope.astype(bf16)
            pre[here, :] = slope
        hid_t[:, part * span : (part + 1) * span] = pre[...].T.astype(bf16)

    for lag in range(1, LAGS + 1):
        at = slice((lag - 1) * latents, lag * latents)
        lagged_out[:, at] = lagged[at, :].astype(f32).T.astype(bf16)
        term = None
        for part in range(parts):
            more = jnp.dot(
                hid_t[:, part * span : (part + 1) * span],
                eff[part][:, at],
                preferred_element_type=f32,
            )
            term = more if term is None else term + more
        term = pltpu.roll(term, rows - lag, 0)
        folded[...] = term if lag == 1 else folded[...] + term
    total = folded[...].T
    if blocks == 1:
        grad_out[0] = total
        return
    for block in range(blocks):
        grad_out[spot(jnp.int32(block))] = total[block * size : (block + 1) * size]
    grad_out[0] += direct_out[...]
    below = spot(jnp.maximum(device - 1, 0))
    above = spot(jnp.minimum(device + 1, blocks - 1))
    for n, at in ((0, below), (1, 0), (2, above)):
        part = slice(n * size, (n + 1) * size)
        values = lat_ref[at]
        window_out[part, :] = values
        grad_out[at] += norm * (values.astype(f32) * sq_ref[part, :] - dec_ref[part, :])


def transition(steps, norm, core, order, inverse, device, lat3, own, bias, out_w, var, dec_sums, squares, eff):
    blocks, size, rows = lat3.shape
    lat_dev, hidden = bias.shape
    span, lag_width = eff[0].shape
    km = lat_dev * hidden
    shape = jax.ShapeDtypeStruct
    return pl.pallas_call(
        functools.partial(transition_kernel, steps, norm, core, order, inverse, len(eff)),
        in_specs=[pl.BlockSpec(memory_space=pltpu.SMEM)] + [VMEM] * (7 + len(eff)),
        out_specs=[VMEM] * 5,
        out_shape=[
            shape((km, rows), bf16),
            shape((rows, lag_width), bf16),
            shape((blocks, size, rows), f32),
            shape((lat_dev, rows), f32),
            shape(dec_sums.shape, bf16),
        ],
        scratch_shapes=[
            pltpu.VMEM((lag_width, rows), bf16),
            pltpu.VMEM((2, span, rows), f32),
            pltpu.VMEM((rows, km), bf16),
            pltpu.VMEM((rows, blocks * size), f32),
        ],
        compiler_params=params(9),
        cost_estimate=pl.CostEstimate(
            flops=4 * km * lag_width * rows,
            bytes_accessed=2 * km * lag_width,
            transcendentals=km * rows,
        ),
        name="transition",
    )(device, lat3, own, bias, out_w, var, dec_sums, squares, *eff)


def weight_kernel(start, hid_ref, lagged_ref, logit_ref, weight_ref, *refs):
    trans_out, graph_out, work = refs[-3:]
    lat_dev, hidden, lag_width = weight_ref.shape
    tile = graph_out.shape[1]
    group = group_of(lat_dev)
    at = pl.multiple_of(start + pl.program_id(0) * tile, tile)
    for g in range(lat_dev // group):
        held = work.at[g % 2]
        held[...] = jnp.dot(
            hid_ref[g * group * hidden : (g + 1) * group * hidden, :],
            lagged_ref[...],
            preferred_element_type=f32,
        )
        latents = slice(g * group, (g + 1) * group)
        edge = jax.nn.sigmoid(logit_ref[latents, :])
        for k in range(group):
            n = g * group + k
            grad = held[k * hidden : (k + 1) * hidden, :]
            trans_out[n] = (grad * edge[k : k + 1]).astype(bf16)
            value = weight_ref[n, :, pl.ds(at, tile)].astype(f32)
            graph_out[n : n + 1, :] = jnp.sum(grad * value, axis=0, keepdims=True)
        flip = edge * (1.0 - edge)
        graph_out[latents, :] = graph_out[latents, :] * flip + sparsity_weight * flip


def weight_grads(hid, lagged, logits, weights, first, count, held):
    lat_dev, hidden, lag_width = weights.shape
    km, rows = hid.shape
    tile = TILE
    group = group_of(lat_dev)
    skip = first // tile
    two = pl.BlockSpec((lat_dev, tile), lambda i: (0, i + skip))
    held = list(held)
    return pl.pallas_call(
        functools.partial(weight_kernel, first),
        grid=(count // tile,),
        in_specs=[
            pl.BlockSpec((km, rows), lambda i: (0, 0)),
            pl.BlockSpec((rows, tile), lambda i: (0, i + skip)),
            two,
            VMEM,
        ]
        + [pl.BlockSpec(memory_space=pl.ANY)] * len(held),
        out_specs=[pl.BlockSpec((lat_dev, hidden, tile), lambda i: (0, 0, i + skip)), two],
        out_shape=[
            jax.ShapeDtypeStruct(weights.shape, bf16),
            jax.ShapeDtypeStruct((lat_dev, lag_width), f32),
        ],
        scratch_shapes=[pltpu.VMEM((2, group * hidden, tile), f32)],
        input_output_aliases={4 + n: n for n in range(len(held))},
        compiler_params=params(16),
        cost_estimate=pl.CostEstimate(
            flops=2 * km * count * rows, bytes_accessed=4 * km * count, transcendentals=0
        ),
        name="weight_grads",
    )(hid, lagged, logits, weights, *held)


TILE = 512


def pick(mask, table, fields):
    both = jnp.dot(table, fields, preferred_element_type=f32)
    return jnp.sum(jnp.where(mask, both, 0.0), axis=0, keepdims=True)


def mask_of(loc_ref, width):
    return lax.broadcasted_iota(jnp.int32, (width, loc_ref.shape[1]), 0) == loc_ref[...]


def grad_dec_kernel(norm, loc_ref, win_ref, dec_ref, fields_ref, out_ref):
    values = win_ref[...]
    mask = mask_of(loc_ref, values.shape[0])
    wide = values.astype(f32)
    power = jnp.sum(wide * wide, axis=1, keepdims=True)
    power = jnp.sum(jnp.where(mask, power, 0.0), axis=0, keepdims=True)
    for var in range(fields_ref.shape[0]):
        cross = pick(mask, values, fields_ref[var])
        out_ref[var : var + 1, :] = norm * (dec_ref[var : var + 1, :] * power - cross)


def grad_enc_kernel(loc_ref, grad_ref, fields_ref, out_ref):
    width = grad_ref.shape[0]
    both = jnp.concatenate([part.astype(bf16) for part in pieces(grad_ref[...], 2)], axis=0)
    mask = mask_of(loc_ref, width)
    for var in range(fields_ref.shape[0]):
        sums = jnp.dot(both, fields_ref[var], preferred_element_type=f32)
        sums = jnp.where(mask, sums[:width] + sums[width:], 0.0)
        out_ref[var : var + 1, :] = jnp.sum(sums, axis=0, keepdims=True)


def cell_call(kernel, loc, table, extras, fields3, name):
    var_count, rows, cells = fields3.shape
    return pl.pallas_call(
        kernel,
        in_specs=[VMEM] * (3 + len(extras)),
        out_specs=VMEM,
        out_shape=jax.ShapeDtypeStruct((var_count, cells), f32),
        compiler_params=params(12),
        cost_estimate=pl.CostEstimate(
            flops=4 * table.shape[0] * rows * cells * var_count,
            bytes_accessed=2 * rows * cells * var_count,
            transcendentals=0,
        ),
        name=name,
    )(loc, table, *extras, fields3)


def paired(block, device, count, first):
    route = []
    for low in range(first, count - 1, 2):
        route += [(low, low + 1), (low + 1, low)]
    return lax.ppermute(block, AXES, route)


def from_neighbours(down, up, device, count):
    even = lax.rem(device, 2) == 0
    first = paired(jnp.where(even, up, down), device, count, 0)
    second = paired(jnp.where(even, down, up), device, count, 1)
    return first, second, even


def body(
    fields,
    cell_latent,
    enc_weight,
    dec_weight,
    trans_weight,
    graph_logits,
    hidden_bias,
    out_weight,
    noise_var,
):
    batch_size, step_count, var_count, cell_count = fields.shape
    lat_dev, hidden, lag_width = trans_weight.shape
    latent_count = lag_width // LAGS
    rows = batch_size * step_count
    norm = 1.0 / rows
    width = 3 * lat_dev
    space, lat = lax.axis_size("space"), lax.axis_size("lat")
    count = space * lat
    device = lax.axis_index(AXES)
    doubling = count & (count - 1) == 0 and lat_dev % 16 == 0
    core = lat.bit_length() - 1
    bits = [n for n in range(count.bit_length() - 2, -1, -1) if n != core]
    bits = list(zip(bits, bits[:-2] + bits[-2:][::-1])) + [(core, core)]

    def swap(pair):
        return [(n, n ^ (1 << pair[(n >> core) & 1])) for n in range(count)]

    loc = (cell_latent - (device - 1) * lat_dev)[None]
    fields3 = jnp.transpose(fields.reshape(rows, var_count, cell_count), (1, 0, 2))
    enc_sums, dec_sums, squares = encode(loc, enc_weight, dec_weight, fields3, width)
    first, second, even = from_neighbours(
        enc_sums[:lat_dev], enc_sums[2 * lat_dev :], device, count
    )
    held_weights = in_vmem(trans_weight)
    parts = lat_dev // group_of(lat_dev)
    eff = []

    def beside(value, after):
        if len(eff) == parts:
            return value
        logits, _ = lax.optimization_barrier((graph_logits, after))
        value, made = lax.optimization_barrier(
            (value, effective(logits, held_weights, len(eff)))
        )
        eff.append(made)
        return value


    own = enc_sums[lat_dev : 2 * lat_dev] + first + second
    own_bf = own.astype(bf16)

    if doubling:
        gathered = own_bf[None]
        for choice in bits:
            got = beside(lax.ppermute(gathered, AXES, swap(choice)), gathered)
            gathered = jnp.concatenate([gathered, got], axis=0)
        order = [[0], [0]]
        for pair in bits:
            came = order if pair[0] != core else order[::-1]
            order = [
                own_order + [n ^ (1 << bit) for n in other]
                for own_order, other, bit in zip(order, came, pair)
            ]
        inverse = [
            (bit, [pair[0] for pair in bits].index(bit), [pair[1] for pair in bits].index(bit))
            for bit, _ in bits
        ]
    else:
        order, inverse = [[0], [0]], []
        gathered = lax.all_gather(own_bf, AXES, axis=0, tiled=True)
        padded = jnp.pad(gathered, ((lat_dev, lat_dev), (0, 0)))
        window = lax.dynamic_slice_in_dim(padded, device * lat_dev, width, 0)
        gathered = gathered[None]

    while len(eff) < parts:
        gathered = beside(gathered, enc_sums)
    eff = [in_vmem(part) for part in eff]
    hid, lagged, partial, direct, seen = transition(
        step_count, norm, core, order, inverse, device.astype(jnp.int32)[None], gathered, own,
        hidden_bias, out_weight, noise_var[None], dec_sums, squares, eff,
    )
    window = seen if doubling else window

    def decoder(values):
        kernel = functools.partial(grad_dec_kernel, norm)
        return cell_call(kernel, loc, values, [dec_weight], fields3, "grad_dec")

    if doubling:
        held, total, done = [], partial, 0
        tiles = lag_width // TILE
        last = tiles // 5
        shares = {1: tiles - 3 * last, 2: last, 3: last}

        def weight_share(n, held, done):
            return weight_grads(
                hid, lagged, graph_logits, held_weights, done * TILE, n * TILE, held
            )

        for n, pair in enumerate(reversed(bits)):
            half = total.shape[0] // 2
            got = lax.ppermute(total[half:].astype(bf16), AXES, swap(pair))
            if n in shares:
                held = weight_share(shares[n], held, done)
                done += shares[n]
                got, held = lax.optimization_barrier((got, held))
            elif n == 4:
                seen, _ = lax.optimization_barrier((window, total))
                got, grad_dec = lax.optimization_barrier((got, decoder(seen)))
            total = total[:half] + got.astype(f32)
        own_grad = total[0]
        hid, own_grad = lax.optimization_barrier((hid, own_grad))
        first, second, even = from_neighbours(own_grad, own_grad, device, count)
        held = weight_share(tiles - done, held, done)
        first, second, held = lax.optimization_barrier((first, second, held))
        grad_trans, grad_graph = held
    else:
        grad_trans, grad_graph = weight_grads(
            hid, lagged, graph_logits, held_weights, 0, lag_width, []
        )
        extra = norm * (window.astype(f32) * squares - dec_sums)
        extra = extra + jnp.pad(direct, ((lat_dev, lat_dev), (0, 0)))
        table = jnp.zeros((latent_count + 2 * lat_dev, rows), f32)
        table = lax.dynamic_update_slice_in_dim(table, extra, device * lat_dev, 0)
        partial = partial[0] + table[lat_dev : lat_dev + latent_count]
        own_grad = lax.psum_scatter(partial, AXES, scatter_dimension=0, tiled=True)
        grad_dec = decoder(window)
        first, second, even = from_neighbours(own_grad, own_grad, device, count)

    grad_window = jnp.concatenate(
        [jnp.where(even, second, first), own_grad, jnp.where(even, first, second)], axis=0
    )
    grad_enc = cell_call(grad_enc_kernel, loc, grad_window, [], fields3, "grad_enc")
    return (grad_enc, grad_dec, grad_trans, grad_graph)


def solution(mesh):
    return jax.shard_map(
        body,
        mesh=mesh,
        in_specs=(
            P(None, None, None, AXES),
            P(AXES),
            P(None, AXES),
            P(None, AXES),
            P(AXES, None, None),
            P(AXES, None),
            P(AXES, None),
            P(AXES, None),
            P(AXES),
        ),
        out_specs=(
            P(None, AXES),
            P(None, AXES),
            P(AXES, None, None),
            P(AXES, None),
        ),
        check_vma=False,
    )
```

```python
import functools

import jax
import jax.numpy as jnp
from jax import lax
from jax.experimental import pallas as pl
from jax.experimental.pallas import tpu as pltpu
from jax.sharding import PartitionSpec as P

LAGS = 5
AXES = ("space", "lat")
sparsity_weight = 0.01
f32 = jnp.float32
bf16 = jnp.bfloat16
MIB = 1 << 20


def params(mib):
    return pltpu.CompilerParams(vmem_limit_bytes=mib * MIB)


def nt_dot(a, b):
    return lax.dot_general(a, b, (((1,), (1,)), ((), ())), preferred_element_type=f32)


def pieces(x, count):
    out = []
    for _ in range(count):
        part = x.astype(bf16)
        out.append(part.astype(f32))
        x = x - out[-1]
    return out


def in_vmem(x):
    return pltpu.with_memory_space_constraint(x, pltpu.VMEM)


VMEM = pl.BlockSpec(memory_space=pltpu.VMEM)


def group_of(lat_dev):
    return 8 if lat_dev % 8 == 0 else lat_dev


def weighted_sums(mask, weight_ref, fields_ref, count):
    width, total = mask.shape[0], None
    for var in range(fields_ref.shape[0]):
        parts = pieces(weight_ref[var : var + 1, :], count)
        parts = [jnp.where(mask, part, 0.0).astype(bf16) for part in parts]
        term = nt_dot(jnp.concatenate(parts, axis=0), fields_ref[var])
        total = term if total is None else total + term
    sums = total[(count - 1) * width :]
    for n in range(count - 2, -1, -1):
        sums = sums + total[n * width : (n + 1) * width]
    return sums


def encode_kernel(loc_ref, enc_ref, fields_ref, enc_out):
    enc_out[...] = weighted_sums(mask_of(loc_ref, enc_out.shape[0]), enc_ref, fields_ref, 3)


def decode_kernel(loc_ref, dec_ref, fields_ref, dec_out, sq_out):
    mask = mask_of(loc_ref, dec_out.shape[0])
    dec_out[...] = weighted_sums(mask, dec_ref, fields_ref, 2)
    square = jnp.sum(dec_ref[...] * dec_ref[...], axis=0, keepdims=True)
    squares = jnp.sum(jnp.where(mask, square, 0.0), axis=1, keepdims=True)
    sq_out[...] = jnp.broadcast_to(squares, sq_out.shape)


def cell_sums(kernel, loc, weight, fields3, width, outs, scale, name):
    var_count, rows, cells = fields3.shape
    return pl.pallas_call(
        kernel,
        in_specs=[VMEM] * 3,
        out_specs=[VMEM] * outs,
        out_shape=[jax.ShapeDtypeStruct((width, rows), f32)] * outs,
        compiler_params=params(12),
        cost_estimate=pl.CostEstimate(
            flops=scale * width * rows * cells * var_count,
            bytes_accessed=2 * rows * cells * var_count,
            transcendentals=0,
        ),
        name=name,
    )(loc, weight, fields3)


def edge_kernel(group, first, logit_ref, weight_ref, out_ref):
    hidden = weight_ref.shape[1]
    for k in range(group):
        edge = jax.nn.sigmoid(logit_ref[first + k : first + k + 1, :])
        out_ref[k * hidden : (k + 1) * hidden, :] = (
            weight_ref[first + k].astype(f32) * edge
        ).astype(bf16)


def effective(logits, weights, part):
    lat_dev, hidden, lag_width = weights.shape
    group = group_of(lat_dev)
    out = pl.pallas_call(
        functools.partial(edge_kernel, group, part * group),
        in_specs=[VMEM] * 2,
        out_specs=VMEM,
        out_shape=jax.ShapeDtypeStruct((group * hidden, lag_width), bf16),
        compiler_params=params(2),
        cost_estimate=pl.CostEstimate(
            flops=2 * group * hidden * lag_width,
            bytes_accessed=4 * group * hidden * lag_width,
            transcendentals=0,
        ),
        name="effective",
    )(logits, weights)
    return in_vmem(out)


def transition_kernel(steps, norm, core, order, inverse, parts, sources, device_ref, own_ref, bias_ref,
                      out_w_ref, var_ref, dec_ref, sq_ref, *refs):
    lat, eff = refs[:sources], refs[sources : sources + parts]
    outs, scratch = refs[sources + parts : -5], refs[-5:]
    hid_out, lagged_out, keep_out, send_out, direct_out, window_out = outs
    lagged, work, hid_t, folded, grad_out = scratch
    half, size, rows = lat[0].shape
    blocks = half * sources
    latents = blocks * size
    span, lag_width = eff[0].shape
    lat_dev, hidden = bias_ref.shape
    group = span // hidden
    device = device_ref[0]
    side = (device >> core) & 1

    def spot(owner):
        away = owner ^ device
        found = jnp.int32(0)
        for bit, first, second in inverse:
            found = found | (((away >> bit) & 1) << jnp.where((owner >> core) & 1, second, first))
        return found

    for p in range(blocks):
        values = lat[p // half][p % half].astype(f32)
        at = pl.multiple_of((device ^ jnp.where(side, order[1][p], order[0][p])) * size, size)
        for lag in range(1, LAGS + 1):
            turned = pltpu.roll(values, lag, 1).astype(bf16)
            lagged[pl.ds((lag - 1) * latents + at, size), :] = turned

    bias_t, out_w_t, var_t = bias_ref[...].T, out_w_ref[...].T, var_ref[...].T
    column = lax.broadcasted_iota(jnp.int32, (group, rows), 1)
    valid = lax.rem(column, steps) >= LAGS
    for part in range(parts):
        pre = work.at[part % 2]
        pre[...] = jnp.dot(eff[part][...], lagged[...], preferred_element_type=f32)
        first = part * group
        for k in range(group):
            value = pre[k * hidden : (k + 1) * hidden, :] + bias_t[:, first + k : first + k + 1]
            out_w = out_w_t[:, first + k : first + k + 1]
            gate = jax.nn.sigmoid(value)
            direct_out[first + k : first + k + 1, :] = jnp.sum(
                value * gate * out_w, axis=0, keepdims=True
            )
            pre[k * hidden : (k + 1) * hidden, :] = out_w * gate * (1.0 + value * (1.0 - gate))
        at = slice(first, first + group)
        direct = norm * (own_ref[at, :] - direct_out[at, :]) / var_t[at, :]
        direct = jnp.where(valid, direct, 0.0)
        direct_out[at, :] = direct
        for k in range(group):
            here = slice(k * hidden, (k + 1) * hidden)
            slope = pre[here, :] * (-direct[k : k + 1, :])
            hid_out[part * span + k * hidden : part * span + (k + 1) * hidden, :] = slope.astype(bf16)
            pre[here, :] = slope
        hid_t[:, part * span : (part + 1) * span] = pre[...].T.astype(bf16)

    for lag in range(1, LAGS + 1):
        at = slice((lag - 1) * latents, lag * latents)
        lagged_out[:, at] = lagged[at, :].astype(f32).T.astype(bf16)
        term = None
        for part in range(parts):
            more = jnp.dot(
                hid_t[:, part * span : (part + 1) * span],
                eff[part][:, at],
                preferred_element_type=f32,
            )
            term = more if term is None else term + more
        term = pltpu.roll(term, rows - lag, 0)
        folded[...] = term if lag == 1 else folded[...] + term
    total = folded[...].T
    if blocks == 1:
        keep_out[0] = total
        send_out[...] = jnp.zeros_like(send_out)
        window_out[...] = jnp.zeros_like(window_out)
        return
    for block in range(blocks):
        grad_out[spot(jnp.int32(block))] = total[block * size : (block + 1) * size]
    grad_out[0] += direct_out[...]
    below = spot(jnp.maximum(device - 1, 0))
    above = spot(jnp.minimum(device + 1, blocks - 1))
    for n, at in ((0, below), (1, 0), (2, above)):
        part = slice(n * size, (n + 1) * size)
        near, far = (source[at & (half - 1)].astype(f32) for source in lat)
        values = jnp.where(at >= half, far, near)
        window_out[part, :] = values.astype(bf16)
        grad_out[at] += norm * (values * sq_ref[part, :] - dec_ref[part, :])
    keep_out[...] = grad_out[:half]
    send_out[...] = grad_out[half:].astype(bf16)


def transition(steps, norm, core, order, inverse, device, lat, own, bias, out_w, var, dec_sums, squares, eff):
    half, size, rows = lat[0].shape
    blocks = half * len(lat)
    lat_dev, hidden = bias.shape
    span, lag_width = eff[0].shape
    km = lat_dev * hidden
    shape = jax.ShapeDtypeStruct
    return pl.pallas_call(
        functools.partial(
            transition_kernel, steps, norm, core, order, inverse, len(eff), len(lat)
        ),
        in_specs=[pl.BlockSpec(memory_space=pltpu.SMEM)] + [VMEM] * (6 + len(lat) + len(eff)),
        out_specs=[VMEM] * 6,
        out_shape=[
            shape((km, rows), bf16),
            shape((rows, lag_width), bf16),
            shape((half, size, rows), f32),
            shape((half, size, rows) if blocks > 1 else (16, rows), bf16),
            shape((lat_dev, rows), f32),
            shape(dec_sums.shape, bf16),
        ],
        scratch_shapes=[
            pltpu.VMEM((lag_width, rows), bf16),
            pltpu.VMEM((2, span, rows), f32),
            pltpu.VMEM((rows, km), bf16),
            pltpu.VMEM((rows, blocks * size), f32),
            pltpu.VMEM((blocks, size, rows), f32),
        ],
        compiler_params=params(8),
        cost_estimate=pl.CostEstimate(
            flops=4 * km * lag_width * rows,
            bytes_accessed=2 * km * lag_width,
            transcendentals=km * rows,
        ),
        name="transition",
    )(device, own, bias, out_w, var, dec_sums, squares, *lat, *eff)


def weight_kernel(start, hid_ref, lagged_ref, logit_ref, weight_ref, *refs):
    trans_out, graph_out, work = refs[-3:]
    lat_dev, hidden, lag_width = weight_ref.shape
    tile = graph_out.shape[1]
    group = group_of(lat_dev)
    at = pl.multiple_of(start + pl.program_id(0) * tile, tile)
    for g in range(lat_dev // group):
        held = work.at[g % 2]
        held[...] = jnp.dot(
            hid_ref[g * group * hidden : (g + 1) * group * hidden, :],
            lagged_ref[...],
            preferred_element_type=f32,
        )
        latents = slice(g * group, (g + 1) * group)
        edge = jax.nn.sigmoid(logit_ref[latents, :])
        for k in range(group):
            n = g * group + k
            grad = held[k * hidden : (k + 1) * hidden, :]
            trans_out[n] = (grad * edge[k : k + 1]).astype(bf16)
            value = weight_ref[n, :, pl.ds(at, tile)].astype(f32)
            graph_out[n : n + 1, :] = jnp.sum(grad * value, axis=0, keepdims=True)
        flip = edge * (1.0 - edge)
        graph_out[latents, :] = graph_out[latents, :] * flip + sparsity_weight * flip


def weight_grads(hid, lagged, logits, weights, first, count, held):
    lat_dev, hidden, lag_width = weights.shape
    km, rows = hid.shape
    tile = TILE
    group = group_of(lat_dev)
    skip = first // tile
    two = pl.BlockSpec((lat_dev, tile), lambda i: (0, i + skip))
    held = list(held)
    return pl.pallas_call(
        functools.partial(weight_kernel, first),
        grid=(count // tile,),
        in_specs=[
            pl.BlockSpec((km, rows), lambda i: (0, 0)),
            pl.BlockSpec((rows, tile), lambda i: (0, i + skip)),
            two,
            VMEM,
        ]
        + [pl.BlockSpec(memory_space=pl.ANY)] * len(held),
        out_specs=[pl.BlockSpec((lat_dev, hidden, tile), lambda i: (0, 0, i + skip)), two],
        out_shape=[
            jax.ShapeDtypeStruct(weights.shape, bf16),
            jax.ShapeDtypeStruct((lat_dev, lag_width), f32),
        ],
        scratch_shapes=[pltpu.VMEM((2, group * hidden, tile), f32)],
        input_output_aliases={4 + n: n for n in range(len(held))},
        compiler_params=params(12),
        cost_estimate=pl.CostEstimate(
            flops=2 * km * count * rows, bytes_accessed=4 * km * count, transcendentals=0
        ),
        name="weight_grads",
    )(hid, lagged, logits, weights, *held)


TILE = 512


def pick(mask, table, fields):
    both = jnp.dot(table, fields, preferred_element_type=f32)
    return jnp.sum(jnp.where(mask, both, 0.0), axis=0, keepdims=True)


def mask_of(loc_ref, width):
    return lax.broadcasted_iota(jnp.int32, (width, loc_ref.shape[1]), 0) == loc_ref[...]


def grad_dec_kernel(norm, loc_ref, win_ref, dec_ref, fields_ref, out_ref):
    values = win_ref[...]
    mask = mask_of(loc_ref, values.shape[0])
    wide = values.astype(f32)
    power = jnp.sum(wide * wide, axis=1, keepdims=True)
    power = jnp.sum(jnp.where(mask, power, 0.0), axis=0, keepdims=True)
    for var in range(fields_ref.shape[0]):
        cross = pick(mask, values, fields_ref[var])
        out_ref[var : var + 1, :] = norm * (dec_ref[var : var + 1, :] * power - cross)


def grad_enc_kernel(loc_ref, grad_ref, fields_ref, out_ref):
    width = grad_ref.shape[0]
    both = jnp.concatenate([part.astype(bf16) for part in pieces(grad_ref[...], 2)], axis=0)
    mask = mask_of(loc_ref, width)
    for var in range(fields_ref.shape[0]):
        sums = jnp.dot(both, fields_ref[var], preferred_element_type=f32)
        sums = jnp.where(mask, sums[:width] + sums[width:], 0.0)
        out_ref[var : var + 1, :] = jnp.sum(sums, axis=0, keepdims=True)


def cell_call(kernel, loc, table, extras, fields3, name):
    var_count, rows, cells = fields3.shape
    return pl.pallas_call(
        kernel,
        in_specs=[VMEM] * (3 + len(extras)),
        out_specs=VMEM,
        out_shape=jax.ShapeDtypeStruct((var_count, cells), f32),
        compiler_params=params(12),
        cost_estimate=pl.CostEstimate(
            flops=4 * table.shape[0] * rows * cells * var_count,
            bytes_accessed=2 * rows * cells * var_count,
            transcendentals=0,
        ),
        name=name,
    )(loc, table, *extras, fields3)


def paired(block, device, count, first):
    route = []
    for low in range(first, count - 1, 2):
        route += [(low, low + 1), (low + 1, low)]
    return lax.ppermute(block, AXES, route)


def from_neighbours(down, up, device, count):
    even = lax.rem(device, 2) == 0
    first = paired(jnp.where(even, up, down), device, count, 0)
    second = paired(jnp.where(even, down, up), device, count, 1)
    return first, second, even


def body(
    fields,
    cell_latent,
    enc_weight,
    dec_weight,
    trans_weight,
    graph_logits,
    hidden_bias,
    out_weight,
    noise_var,
):
    batch_size, step_count, var_count, cell_count = fields.shape
    lat_dev, hidden, lag_width = trans_weight.shape
    latent_count = lag_width // LAGS
    rows = batch_size * step_count
    norm = 1.0 / rows
    width = 3 * lat_dev
    space, lat = lax.axis_size("space"), lax.axis_size("lat")
    count = space * lat
    device = lax.axis_index(AXES)
    doubling = count & (count - 1) == 0 and lat_dev % 16 == 0
    core = lat.bit_length() - 1
    bits = [n for n in range(count.bit_length() - 2, -1, -1) if n != core]
    bits = list(zip(bits, bits[:-2] + bits[-2:][::-1])) + [(core, core)]

    def swap(pair):
        return [(n, n ^ (1 << pair[(n >> core) & 1])) for n in range(count)]

    loc = (cell_latent - (device - 1) * lat_dev)[None]
    fields3 = jnp.transpose(fields.reshape(rows, var_count, cell_count), (1, 0, 2))
    (enc_sums,) = cell_sums(encode_kernel, loc, enc_weight, fields3, width, 1, 80, "encode")
    loc_later, _ = lax.optimization_barrier((loc, enc_sums))
    dec_sums, squares = cell_sums(
        decode_kernel, loc_later, dec_weight, fields3, width, 2, 50, "decode"
    )
    first, second, even = from_neighbours(
        enc_sums[:lat_dev], enc_sums[2 * lat_dev :], device, count
    )
    held_weights = in_vmem(trans_weight)
    parts = lat_dev // group_of(lat_dev)
    eff = []

    def beside(value, after):
        if len(eff) == parts:
            return value
        logits, _ = lax.optimization_barrier((graph_logits, after))
        value, made = lax.optimization_barrier(
            (value, effective(logits, held_weights, len(eff)))
        )
        eff.append(made)
        return value


    first, second, dec_sums = lax.optimization_barrier((first, second, dec_sums))
    own = enc_sums[lat_dev : 2 * lat_dev] + first + second
    own_bf = own.astype(bf16)

    def transposed(after):
        late, _ = lax.optimization_barrier((fields, after))
        return jnp.transpose(late.reshape(rows, var_count, cell_count), (1, 0, 2))

    fields_late = fields3
    if doubling:
        gathered = own_bf[None]
        for choice in bits:
            got = beside(lax.ppermute(gathered, AXES, swap(choice)), gathered)
            halves = [gathered, got]
            if choice != bits[-1]:
                gathered = jnp.concatenate(halves, axis=0)
        order = [[0], [0]]
        for pair in bits:
            came = order if pair[0] != core else order[::-1]
            order = [
                own_order + [n ^ (1 << bit) for n in other]
                for own_order, other, bit in zip(order, came, pair)
            ]
        inverse = [
            (bit, [pair[0] for pair in bits].index(bit), [pair[1] for pair in bits].index(bit))
            for bit, _ in bits
        ]
    else:
        order, inverse = [[0], [0]], []
        gathered = lax.all_gather(own_bf, AXES, axis=0, tiled=True)
        padded = jnp.pad(gathered, ((lat_dev, lat_dev), (0, 0)))
        window = lax.dynamic_slice_in_dim(padded, device * lat_dev, width, 0)
        halves = [gathered[None]]

    while len(eff) < parts:
        halves[0] = beside(halves[0], enc_sums)
    eff = [in_vmem(part) for part in eff]
    hid, lagged, partial, sent, direct, seen = transition(
        step_count, norm, core, order, inverse, device.astype(jnp.int32)[None], halves, own,
        hidden_bias, out_weight, noise_var[None], dec_sums, squares, eff,
    )
    window = seen if doubling else window

    def decoder(values):
        kernel = functools.partial(grad_dec_kernel, norm)
        return cell_call(kernel, loc, values, [dec_weight], fields_late, "grad_dec")

    if doubling:
        held, total, done = [], partial, 0
        tiles = lag_width // TILE
        last = tiles // 5
        shares = {1: tiles - 3 * last, 2: last, 3: last}

        def weight_share(n, held, done):
            return weight_grads(
                hid, lagged, graph_logits, held_weights, done * TILE, n * TILE, held
            )

        for n, pair in enumerate(reversed(bits)):
            if n == 1:
                fields_late = transposed(total)
            if n > 0:
                half = total.shape[0] // 2
                total, sent = total[:half], total[half:].astype(bf16)
            got = lax.ppermute(sent, AXES, swap(pair))
            if n == 1:
                got, fields_late = lax.optimization_barrier((got, fields_late))
            if n in shares:
                held = weight_share(shares[n], held, done)
                done += shares[n]
                got, held = lax.optimization_barrier((got, held))
            elif n == 4:
                seen, _ = lax.optimization_barrier((window, total))
                got, grad_dec = lax.optimization_barrier((got, decoder(seen)))
            total = total + got.astype(f32)
        own_grad = total[0]
        hid, own_grad = lax.optimization_barrier((hid, own_grad))
        first, second, even = from_neighbours(own_grad, own_grad, device, count)
        held = weight_share(tiles - done, held, done)
        first, second, held = lax.optimization_barrier((first, second, held))
        grad_trans, grad_graph = held
    else:
        grad_trans, grad_graph = weight_grads(
            hid, lagged, graph_logits, held_weights, 0, lag_width, []
        )
        extra = norm * (window.astype(f32) * squares - dec_sums)
        extra = extra + jnp.pad(direct, ((lat_dev, lat_dev), (0, 0)))
        table = jnp.zeros((latent_count + 2 * lat_dev, rows), f32)
        table = lax.dynamic_update_slice_in_dim(table, extra, device * lat_dev, 0)
        partial = partial[0] + table[lat_dev : lat_dev + latent_count]
        own_grad = lax.psum_scatter(partial, AXES, scatter_dimension=0, tiled=True)
        grad_dec = decoder(window)
        first, second, even = from_neighbours(own_grad, own_grad, device, count)

    grad_window = jnp.concatenate(
        [jnp.where(even, second, first), own_grad, jnp.where(even, first, second)], axis=0
    )
    grad_enc = cell_call(grad_enc_kernel, loc, grad_window, [], fields_late, "grad_enc")
    return (grad_enc, grad_dec, grad_trans, grad_graph)


def solution(mesh):
    return jax.shard_map(
        body,
        mesh=mesh,
        in_specs=(
            P(None, None, None, AXES),
            P(AXES),
            P(None, AXES),
            P(None, AXES),
            P(AXES, None, None),
            P(AXES, None),
            P(AXES, None),
            P(AXES, None),
            P(AXES),
        ),
        out_specs=(
            P(None, AXES),
            P(None, AXES),
            P(AXES, None, None),
            P(AXES, None),
        ),
        check_vma=False,
    )
```

```python
import functools

import jax
import jax.numpy as jnp
from jax import lax
from jax.experimental import pallas as pl
from jax.experimental.pallas import tpu as pltpu
from jax.sharding import PartitionSpec as P

LAGS = 5
AXES = ("space", "lat")
sparsity_weight = 0.01
f32 = jnp.float32
bf16 = jnp.bfloat16
MIB = 1 << 20


def params(mib):
    return pltpu.CompilerParams(vmem_limit_bytes=mib * MIB)


def nt_dot(a, b):
    return lax.dot_general(a, b, (((1,), (1,)), ((), ())), preferred_element_type=f32)


def pieces(x, count):
    out = []
    for _ in range(count):
        part = x.astype(bf16)
        out.append(part.astype(f32))
        x = x - out[-1]
    return out


def in_vmem(x):
    return pltpu.with_memory_space_constraint(x, pltpu.VMEM)


VMEM = pl.BlockSpec(memory_space=pltpu.VMEM)


def group_of(lat_dev):
    return 8 if lat_dev % 8 == 0 else lat_dev


def weighted_sums(mask, weight_ref, fields_ref, count):
    width, total = mask.shape[0], None
    for var in range(fields_ref.shape[0]):
        parts = pieces(weight_ref[var : var + 1, :], count)
        parts = [jnp.where(mask, part, 0.0).astype(bf16) for part in parts]
        term = nt_dot(jnp.concatenate(parts, axis=0), fields_ref[var])
        total = term if total is None else total + term
    sums = total[(count - 1) * width :]
    for n in range(count - 2, -1, -1):
        sums = sums + total[n * width : (n + 1) * width]
    return sums


def encode_kernel(loc_ref, enc_ref, fields_ref, enc_out):
    enc_out[...] = weighted_sums(mask_of(loc_ref, enc_out.shape[0]), enc_ref, fields_ref, 3)


def decode_kernel(loc_ref, dec_ref, fields_ref, dec_out, sq_out):
    mask = mask_of(loc_ref, dec_out.shape[0])
    dec_out[...] = weighted_sums(mask, dec_ref, fields_ref, 2)
    square = jnp.sum(dec_ref[...] * dec_ref[...], axis=0, keepdims=True)
    squares = jnp.sum(jnp.where(mask, square, 0.0), axis=1, keepdims=True)
    sq_out[...] = jnp.broadcast_to(squares, sq_out.shape)


def cell_sums(kernel, loc, weight, fields3, width, outs, scale, name):
    var_count, rows, cells = fields3.shape
    return pl.pallas_call(
        kernel,
        in_specs=[VMEM] * 3,
        out_specs=[VMEM] * outs,
        out_shape=[jax.ShapeDtypeStruct((width, rows), f32)] * outs,
        compiler_params=params(12),
        cost_estimate=pl.CostEstimate(
            flops=scale * width * rows * cells * var_count,
            bytes_accessed=2 * rows * cells * var_count,
            transcendentals=0,
        ),
        name=name,
    )(loc, weight, fields3)


def edge_kernel(group, first, logit_ref, weight_ref, out_ref):
    hidden = weight_ref.shape[1]
    for k in range(group):
        edge = jax.nn.sigmoid(logit_ref[first + k : first + k + 1, :])
        out_ref[k * hidden : (k + 1) * hidden, :] = (
            weight_ref[first + k].astype(f32) * edge
        ).astype(bf16)


def effective(logits, weights, part):
    lat_dev, hidden, lag_width = weights.shape
    group = group_of(lat_dev)
    out = pl.pallas_call(
        functools.partial(edge_kernel, group, part * group),
        in_specs=[VMEM] * 2,
        out_specs=VMEM,
        out_shape=jax.ShapeDtypeStruct((group * hidden, lag_width), bf16),
        compiler_params=params(2),
        cost_estimate=pl.CostEstimate(
            flops=2 * group * hidden * lag_width,
            bytes_accessed=4 * group * hidden * lag_width,
            transcendentals=0,
        ),
        name="effective",
    )(logits, weights)
    return in_vmem(out)


def transition_kernel(steps, norm, core, order, inverse, parts, sources, device_ref, own_ref, bias_ref,
                      out_w_ref, var_ref, dec_ref, sq_ref, *refs):
    lat, eff = refs[:sources], refs[sources : sources + parts]
    outs, scratch = refs[sources + parts : -5], refs[-5:]
    hid_out, lagged_out, keep_out, send_out, direct_out, window_out = outs
    lagged, work, hid_t, folded, grad_out = scratch
    half, size, rows = lat[0].shape
    blocks = half * sources
    latents = blocks * size
    span, lag_width = eff[0].shape
    lat_dev, hidden = bias_ref.shape
    group = span // hidden
    device = device_ref[0]
    side = (device >> core) & 1

    def spot(owner):
        away = owner ^ device
        found = jnp.int32(0)
        for bit, first, second in inverse:
            found = found | (((away >> bit) & 1) << jnp.where((owner >> core) & 1, second, first))
        return found

    for p in range(blocks):
        values = lat[p // half][p % half].astype(f32)
        at = 0
        if blocks > 1:
            owner = device ^ jnp.where(side, order[1][p], order[0][p])
            at = pl.multiple_of(owner * size, size)
        for lag in range(1, LAGS + 1):
            turned = pltpu.roll(values, lag, 1).astype(bf16)
            lagged[pl.ds((lag - 1) * latents + at, size), :] = turned

    bias_t, out_w_t, var_t = bias_ref[...].T, out_w_ref[...].T, var_ref[...].T
    column = lax.broadcasted_iota(jnp.int32, (group, rows), 1)
    valid = lax.rem(column, steps) >= LAGS
    for part in range(parts):
        pre = work.at[part % 2]
        pre[...] = jnp.dot(eff[part][...], lagged[...], preferred_element_type=f32)
        first = part * group
        for k in range(group):
            value = pre[k * hidden : (k + 1) * hidden, :] + bias_t[:, first + k : first + k + 1]
            out_w = out_w_t[:, first + k : first + k + 1]
            gate = jax.nn.sigmoid(value)
            direct_out[first + k : first + k + 1, :] = jnp.sum(
                value * gate * out_w, axis=0, keepdims=True
            )
            pre[k * hidden : (k + 1) * hidden, :] = out_w * gate * (1.0 + value * (1.0 - gate))
        at = slice(first, first + group)
        direct = norm * (own_ref[at, :] - direct_out[at, :]) / var_t[at, :]
        direct = jnp.where(valid, direct, 0.0)
        direct_out[at, :] = direct
        for k in range(group):
            here = slice(k * hidden, (k + 1) * hidden)
            slope = pre[here, :] * (-direct[k : k + 1, :])
            hid_out[part * span + k * hidden : part * span + (k + 1) * hidden, :] = slope.astype(bf16)
            pre[here, :] = slope
        hid_t[:, part * span : (part + 1) * span] = pre[...].T.astype(bf16)

    for lag in range(1, LAGS + 1):
        at = slice((lag - 1) * latents, lag * latents)
        lagged_out[:, at] = lagged[at, :].astype(f32).T.astype(bf16)
        term = None
        for part in range(parts):
            more = jnp.dot(
                hid_t[:, part * span : (part + 1) * span],
                eff[part][:, at],
                preferred_element_type=f32,
            )
            term = more if term is None else term + more
        term = pltpu.roll(term, rows - lag, 0)
        folded[...] = term if lag == 1 else folded[...] + term
    total = folded[...].T
    if blocks == 1:
        keep_out[0] = total
        send_out[...] = jnp.zeros_like(send_out)
        window_out[...] = jnp.zeros_like(window_out)
        return
    for block in range(blocks):
        grad_out[spot(jnp.int32(block))] = total[block * size : (block + 1) * size]
    grad_out[0] += direct_out[...]
    below = spot(jnp.maximum(device - 1, 0))
    above = spot(jnp.minimum(device + 1, blocks - 1))
    for n, at in ((0, below), (1, 0), (2, above)):
        part = slice(n * size, (n + 1) * size)
        near, far = (source[at & (half - 1)].astype(f32) for source in lat)
        values = jnp.where(at >= half, far, near)
        window_out[part, :] = values.astype(bf16)
        grad_out[at] += norm * (values * sq_ref[part, :] - dec_ref[part, :])
    keep_out[...] = grad_out[:half]
    send_out[...] = grad_out[half:].astype(bf16)


def transition(steps, norm, core, order, inverse, device, lat, own, bias, out_w, var, dec_sums, squares, eff):
    half, size, rows = lat[0].shape
    blocks = half * len(lat)
    lat_dev, hidden = bias.shape
    span, lag_width = eff[0].shape
    km = lat_dev * hidden
    shape = jax.ShapeDtypeStruct
    return pl.pallas_call(
        functools.partial(
            transition_kernel, steps, norm, core, order, inverse, len(eff), len(lat)
        ),
        in_specs=[pl.BlockSpec(memory_space=pltpu.SMEM)] + [VMEM] * (6 + len(lat) + len(eff)),
        out_specs=[VMEM] * 6,
        out_shape=[
            shape((km, rows), bf16),
            shape((rows, lag_width), bf16),
            shape((half, size, rows), f32),
            shape((half, size, rows) if blocks > 1 else (16, rows), bf16),
            shape((lat_dev, rows), f32),
            shape(dec_sums.shape, bf16),
        ],
        scratch_shapes=[
            pltpu.VMEM((lag_width, rows), bf16),
            pltpu.VMEM((2, span, rows), f32),
            pltpu.VMEM((rows, km), bf16),
            pltpu.VMEM((rows, blocks * size), f32),
            pltpu.VMEM((blocks, size, rows), f32),
        ],
        compiler_params=params(8),
        cost_estimate=pl.CostEstimate(
            flops=4 * km * lag_width * rows,
            bytes_accessed=2 * km * lag_width,
            transcendentals=km * rows,
        ),
        name="transition",
    )(device, own, bias, out_w, var, dec_sums, squares, *lat, *eff)


def weight_kernel(start, hid_ref, lagged_ref, logit_ref, weight_ref, *refs):
    trans_out, graph_out, work = refs[-3:]
    lat_dev, hidden, lag_width = weight_ref.shape
    tile = graph_out.shape[1]
    group = group_of(lat_dev)
    at = pl.multiple_of(start + pl.program_id(0) * tile, tile)
    for g in range(lat_dev // group):
        held = work.at[g % 2]
        held[...] = jnp.dot(
            hid_ref[g * group * hidden : (g + 1) * group * hidden, :],
            lagged_ref[...],
            preferred_element_type=f32,
        )
        latents = slice(g * group, (g + 1) * group)
        edge = jax.nn.sigmoid(logit_ref[latents, :])
        for k in range(group):
            n = g * group + k
            grad = held[k * hidden : (k + 1) * hidden, :]
            trans_out[n] = (grad * edge[k : k + 1]).astype(bf16)
            value = weight_ref[n, :, pl.ds(at, tile)].astype(f32)
            graph_out[n : n + 1, :] = jnp.sum(grad * value, axis=0, keepdims=True)
        flip = edge * (1.0 - edge)
        graph_out[latents, :] = graph_out[latents, :] * flip + sparsity_weight * flip


def weight_grads(hid, lagged, logits, weights, first, count, held):
    lat_dev, hidden, lag_width = weights.shape
    km, rows = hid.shape
    tile = TILE
    group = group_of(lat_dev)
    skip = first // tile
    two = pl.BlockSpec((lat_dev, tile), lambda i: (0, i + skip))
    held = list(held)
    return pl.pallas_call(
        functools.partial(weight_kernel, first),
        grid=(count // tile,),
        in_specs=[
            pl.BlockSpec((km, rows), lambda i: (0, 0)),
            pl.BlockSpec((rows, tile), lambda i: (0, i + skip)),
            two,
            VMEM,
        ]
        + [pl.BlockSpec(memory_space=pl.ANY)] * len(held),
        out_specs=[pl.BlockSpec((lat_dev, hidden, tile), lambda i: (0, 0, i + skip)), two],
        out_shape=[
            jax.ShapeDtypeStruct(weights.shape, bf16),
            jax.ShapeDtypeStruct((lat_dev, lag_width), f32),
        ],
        scratch_shapes=[pltpu.VMEM((2, group * hidden, tile), f32)],
        input_output_aliases={4 + n: n for n in range(len(held))},
        compiler_params=params(12),
        cost_estimate=pl.CostEstimate(
            flops=2 * km * count * rows, bytes_accessed=4 * km * count, transcendentals=0
        ),
        name="weight_grads",
    )(hid, lagged, logits, weights, *held)


TILE = 512


def pick(mask, table, fields):
    both = jnp.dot(table, fields, preferred_element_type=f32)
    return jnp.sum(jnp.where(mask, both, 0.0), axis=0, keepdims=True)


def mask_of(loc_ref, width):
    return lax.broadcasted_iota(jnp.int32, (width, loc_ref.shape[1]), 0) == loc_ref[...]


def grad_dec_kernel(norm, loc_ref, win_ref, dec_ref, fields_ref, out_ref):
    values = win_ref[...]
    mask = mask_of(loc_ref, values.shape[0])
    wide = values.astype(f32)
    power = jnp.sum(wide * wide, axis=1, keepdims=True)
    power = jnp.sum(jnp.where(mask, power, 0.0), axis=0, keepdims=True)
    for var in range(fields_ref.shape[0]):
        cross = pick(mask, values, fields_ref[var])
        out_ref[var : var + 1, :] = norm * (dec_ref[var : var + 1, :] * power - cross)


def grad_enc_kernel(loc_ref, grad_ref, fields_ref, out_ref):
    width = grad_ref.shape[0]
    both = jnp.concatenate([part.astype(bf16) for part in pieces(grad_ref[...], 2)], axis=0)
    mask = mask_of(loc_ref, width)
    for var in range(fields_ref.shape[0]):
        sums = jnp.dot(both, fields_ref[var], preferred_element_type=f32)
        sums = jnp.where(mask, sums[:width] + sums[width:], 0.0)
        out_ref[var : var + 1, :] = jnp.sum(sums, axis=0, keepdims=True)


def cell_call(kernel, loc, table, extras, fields3, name):
    var_count, rows, cells = fields3.shape
    return pl.pallas_call(
        kernel,
        in_specs=[VMEM] * (3 + len(extras)),
        out_specs=VMEM,
        out_shape=jax.ShapeDtypeStruct((var_count, cells), f32),
        compiler_params=params(12),
        cost_estimate=pl.CostEstimate(
            flops=4 * table.shape[0] * rows * cells * var_count,
            bytes_accessed=2 * rows * cells * var_count,
            transcendentals=0,
        ),
        name=name,
    )(loc, table, *extras, fields3)


def paired(block, device, count, first):
    route = []
    for low in range(first, count - 1, 2):
        route += [(low, low + 1), (low + 1, low)]
    return lax.ppermute(block, AXES, route)


def from_neighbours(down, up, device, count):
    even = lax.rem(device, 2) == 0
    first = paired(jnp.where(even, up, down), device, count, 0)
    second = paired(jnp.where(even, down, up), device, count, 1)
    return first, second, even


def body(
    fields,
    cell_latent,
    enc_weight,
    dec_weight,
    trans_weight,
    graph_logits,
    hidden_bias,
    out_weight,
    noise_var,
):
    batch_size, step_count, var_count, cell_count = fields.shape
    lat_dev, hidden, lag_width = trans_weight.shape
    latent_count = lag_width // LAGS
    rows = batch_size * step_count
    norm = 1.0 / rows
    width = 3 * lat_dev
    space, lat = lax.axis_size("space"), lax.axis_size("lat")
    count = space * lat
    device = lax.axis_index(AXES)
    doubling = count & (count - 1) == 0 and lat_dev % 16 == 0
    core = lat.bit_length() - 1
    bits = [n for n in range(count.bit_length() - 2, -1, -1) if n != core]
    bits = list(zip(bits, bits[:-2] + bits[-2:][::-1])) + [(core, core)]

    def swap(pair):
        return [(n, n ^ (1 << pair[(n >> core) & 1])) for n in range(count)]

    loc = (cell_latent - (device - 1) * lat_dev)[None]
    fields3 = jnp.transpose(fields.reshape(rows, var_count, cell_count), (1, 0, 2))
    (enc_sums,) = cell_sums(encode_kernel, loc, enc_weight, fields3, width, 1, 80, "encode")
    loc_later, _ = lax.optimization_barrier((loc, enc_sums))
    dec_sums, squares = cell_sums(
        decode_kernel, loc_later, dec_weight, fields3, width, 2, 50, "decode"
    )
    first, second, even = from_neighbours(
        enc_sums[:lat_dev], enc_sums[2 * lat_dev :], device, count
    )
    held_weights = in_vmem(trans_weight)
    parts = lat_dev // group_of(lat_dev)
    eff = []

    def beside(value, after):
        if len(eff) == parts:
            return value
        logits, _ = lax.optimization_barrier((graph_logits, after))
        value, made = lax.optimization_barrier(
            (value, effective(logits, held_weights, len(eff)))
        )
        eff.append(made)
        return value


    first, second, dec_sums = lax.optimization_barrier((first, second, dec_sums))
    own = enc_sums[lat_dev : 2 * lat_dev] + first + second
    own_bf = own.astype(bf16)

    def transposed(after):
        late, _ = lax.optimization_barrier((fields, after))
        return jnp.transpose(late.reshape(rows, var_count, cell_count), (1, 0, 2))

    fields_late = fields3
    if doubling:
        gathered = own_bf[None]
        for choice in bits:
            got = beside(lax.ppermute(gathered, AXES, swap(choice)), gathered)
            halves = [gathered, got]
            if choice != bits[-1]:
                gathered = jnp.concatenate(halves, axis=0)
        order = [[0], [0]]
        for pair in bits:
            came = order if pair[0] != core else order[::-1]
            order = [
                own_order + [n ^ (1 << bit) for n in other]
                for own_order, other, bit in zip(order, came, pair)
            ]
        inverse = [
            (bit, [pair[0] for pair in bits].index(bit), [pair[1] for pair in bits].index(bit))
            for bit, _ in bits
        ]
    else:
        order, inverse = [[0], [0]], []
        gathered = lax.all_gather(own_bf, AXES, axis=0, tiled=True)
        padded = jnp.pad(gathered, ((lat_dev, lat_dev), (0, 0)))
        window = lax.dynamic_slice_in_dim(padded, device * lat_dev, width, 0)
        halves = [gathered[None]]

    while len(eff) < parts:
        halves[0] = beside(halves[0], enc_sums)
    eff = [in_vmem(part) for part in eff]
    hid, lagged, partial, sent, direct, seen = transition(
        step_count, norm, core, order, inverse, device.astype(jnp.int32)[None], halves, own,
        hidden_bias, out_weight, noise_var[None], dec_sums, squares, eff,
    )
    window = seen if doubling else window

    def decoder(values):
        kernel = functools.partial(grad_dec_kernel, norm)
        return cell_call(kernel, loc, values, [dec_weight], fields_late, "grad_dec")

    if doubling:
        held, total, done = [], partial, 0
        tiles = lag_width // TILE
        last = tiles // 5
        shares = {1: tiles - 3 * last, 2: last, 3: last}

        def weight_share(n, held, done):
            return weight_grads(
                hid, lagged, graph_logits, held_weights, done * TILE, n * TILE, held
            )

        for n, pair in enumerate(reversed(bits)):
            if n == 1:
                fields_late = transposed(total)
            if n > 0:
                half = total.shape[0] // 2
                total, sent = total[:half], total[half:].astype(bf16)
            got = lax.ppermute(sent, AXES, swap(pair))
            if n == 1:
                got, fields_late = lax.optimization_barrier((got, fields_late))
            if n in shares:
                held = weight_share(shares[n], held, done)
                done += shares[n]
                got, held = lax.optimization_barrier((got, held))
            elif n == 4:
                seen, _ = lax.optimization_barrier((window, total))
                got, grad_dec = lax.optimization_barrier((got, decoder(seen)))
            total = total + got.astype(f32)
        own_grad = total[0]
        hid, own_grad = lax.optimization_barrier((hid, own_grad))
        first, second, even = from_neighbours(own_grad, own_grad, device, count)
        held = weight_share(tiles - done, held, done)
        first, second, held = lax.optimization_barrier((first, second, held))
        grad_trans, grad_graph = held
    else:
        grad_trans, grad_graph = weight_grads(
            hid, lagged, graph_logits, held_weights, 0, lag_width, []
        )
        extra = norm * (window.astype(f32) * squares - dec_sums)
        extra = extra + jnp.pad(direct, ((lat_dev, lat_dev), (0, 0)))
        table = jnp.zeros((latent_count + 2 * lat_dev, rows), f32)
        table = lax.dynamic_update_slice_in_dim(table, extra, device * lat_dev, 0)
        partial = partial[0] + table[lat_dev : lat_dev + latent_count]
        own_grad = lax.psum_scatter(partial, AXES, scatter_dimension=0, tiled=True)
        grad_dec = decoder(window)
        first, second, even = from_neighbours(own_grad, own_grad, device, count)

    grad_window = jnp.concatenate(
        [jnp.where(even, second, first), own_grad, jnp.where(even, first, second)], axis=0
    )
    grad_enc = cell_call(grad_enc_kernel, loc, grad_window, [], fields_late, "grad_enc")
    return (grad_enc, grad_dec, grad_trans, grad_graph)


def solution(mesh):
    return jax.shard_map(
        body,
        mesh=mesh,
        in_specs=(
            P(None, None, None, AXES),
            P(AXES),
            P(None, AXES),
            P(None, AXES),
            P(AXES, None, None),
            P(AXES, None),
            P(AXES, None),
            P(AXES, None),
            P(AXES),
        ),
        out_specs=(
            P(None, AXES),
            P(None, AXES),
            P(AXES, None, None),
            P(AXES, None),
        ),
        check_vma=False,
    )
```
